256 devices in a mesh: seq: 16 (over x, y), head: 16 (over z, core).
Axes of the slice: x: 4, y: 4, z: 8, core: 2. Of those that a mesh axis runs over, the one named last changes fastest.
Arguments:
- video_rows: bfloat16 [8192, 5120], P('seq'), may hold values from -6 to 6
- context: bfloat16 [512, 5120], P('seq'), may hold values from -6 to 6
- valid_length: int32 [1], replicated, may hold values from 64 to 512
- timestep: int32 [1], replicated, may hold values from 0 to 999
- query_weight: bfloat16 [5120, 4096], P('seq', 'head'), may hold values from -0.078125 to 0.078125
- key_weight: bfloat16 [5120, 4096], P('seq', 'head'), may hold values from -0.078125 to 0.078125
- value_weight: bfloat16 [5120, 4096], P('seq', 'head'), may hold values from -0.078125 to 0.078125
- out_weight: bfloat16 [4096, 5120], P('head', 'seq'), may hold values from -0.09375 to 0.09375
- query_gain: float32 [4096], P('head'), may hold values from 0.5 to 15
- key_gain: float32 [4096], P('head'), may hold values from 0.5 to 15
- time_weight: bfloat16 [2, 256, 5120], P(None, None, 'head'), may hold values from -0.375 to 0.375
- modulation: float32 [2, 5120], P(None, 'head'), may hold values from -3 to 3
Outputs:
- residual_out: bfloat16 [8192, 5120], P('seq', 'head')
- modulated: bfloat16 [8192, 5120], P('seq', 'head')
The draws below stay inside these ranges and needn't reach their ends.
Inputs may be any that keep to these rules, and one draw needn't show every extreme that they name: `valid_length`: text positions at or beyond it are padding.
All inputs are finite; a program needn't handle non-finite values.
Results may differ from the reference program's by a relative error of at most 0.0065.
The reference program's roundings to bfloat16 on the way (of `normed`, `value_proj`, `query_normed`, `key_normed`, `weights`, `attended` and `act`) count: a program that leaves them out, or rounds other values in their place, can miss the bound.
Values may be sent and summed in bfloat16 or wider, within the bound.
A program may use at most 64 MiB of HBM per device.

```python
import jax
import jax.numpy as jnp
from jax import lax

D = 5120
HD = 128
TEXT = 512
FREQ = 256
HEADS = 32
ATT = 4096
TOKENS = 8192


def head_gains(key):
    base = jax.random.uniform(key, (HEADS, HD), jnp.float32, 0.5, 1.5)
    return base.reshape(HEADS * HD)


def draw_query_gain(key, part):
    return head_gains(jax.random.fold_in(key, 11))


def draw_key_gain(key, part):
    return head_gains(jax.random.fold_in(key, 23))


def shard_levels(rng, shape, cuts, least, top_value):
    def one(axis_at, parts):
        steps = jax.random.uniform(jax.random.fold_in(jax.random.fold_in(rng, 6), axis_at), (parts,), jnp.float32, least / len(cuts), top_value / len(cuts))
        return jnp.repeat(jnp.exp(steps), shape[axis_at] // parts).reshape((-1,) + (1,) * (len(shape) - axis_at - 1))

    loudness = one(*cuts[0])
    for cut in cuts[1:]:
        loudness = loudness * one(*cut)
    return loudness


def centred(own_key, shape, deviation, limit, pieces=(), held_as=jnp.bfloat16):
    loudness = shard_levels(own_key, shape, pieces, -0.22, 0.18) if pieces else 1.0
    entries = jax.random.normal(own_key, shape, jnp.float32) * deviation * loudness
    return jnp.minimum(jnp.maximum(entries, -limit), limit).astype(held_as)


def setup_inputs(seed: int = 0) -> dict:
    arg_keys = jax.random.split(jax.random.key(seed), 13)
    video_rows = centred(arg_keys[0], (TOKENS, D), 1.0, 6.0, ((0, 16),))
    context = centred(arg_keys[1], (TEXT, D), 1.0, 6.0, ((0, 16),))
    valid_length = jax.random.randint(arg_keys[2], (1,), TEXT // 8, TEXT + 1).astype(jnp.int32)
    timestep = jax.random.randint(arg_keys[3], (1,), 0, 1000).astype(jnp.int32)
    query_weight = centred(arg_keys[4], (D, ATT), D ** -0.5, 0.078125, ((0, 16), (1, 16)))
    key_weight = centred(arg_keys[5], (D, ATT), D ** -0.5, 0.078125, ((0, 16), (1, 16)))
    value_weight = centred(arg_keys[6], (D, ATT), D ** -0.5, 0.078125, ((0, 16), (1, 16)))
    out_weight = centred(arg_keys[7], (ATT, D), ATT ** -0.5, 0.09375, ((0, 16), (1, 16)))
    query_gain = draw_query_gain(jax.random.fold_in(arg_keys[12], 71), 0)
    key_gain = draw_key_gain(jax.random.fold_in(arg_keys[12], 71), 0)
    time_weight = centred(arg_keys[10], (2, FREQ, D), FREQ ** -0.5, 0.375, ((2, 16),))
    modulation = centred(arg_keys[11], (2, D), 0.5, 3.0, ((1, 16),), jnp.float32)
    return {"video_rows": video_rows, "context": context, "valid_length": valid_length, "timestep": timestep, "query_weight": query_weight, "key_weight": key_weight, "value_weight": value_weight, "out_weight": out_weight, "query_gain": query_gain, "key_gain": key_gain, "time_weight": time_weight, "modulation": modulation}


def layer_norm(rows):
    mean = lax.optimization_barrier(jnp.mean(rows, axis=-1, keepdims=True))
    spread = lax.optimization_barrier(jnp.mean((rows - mean) ** 2, axis=-1, keepdims=True))
    return (rows - mean) / jnp.sqrt(spread + 1e-06)

def rms_gain(rows, gain):
    return rows / jnp.sqrt(lax.optimization_barrier(jnp.mean(rows * rows, axis=-1, keepdims=True)) + 1e-06) * gain

def reference(video_rows, context, valid_length, timestep, query_weight, key_weight, value_weight, out_weight, query_gain, key_gain, time_weight, modulation):
    normed = layer_norm(video_rows.astype(jnp.float32)).astype(jnp.bfloat16)
    queries = jnp.dot(normed, query_weight, preferred_element_type=jnp.float32)
    key_proj = jnp.dot(context, key_weight, preferred_element_type=jnp.float32)
    value_proj = jnp.dot(context, value_weight, preferred_element_type=jnp.float32).astype(jnp.bfloat16)
    query_normed = rms_gain(queries, query_gain).astype(jnp.bfloat16)
    key_normed = rms_gain(key_proj, key_gain).astype(jnp.bfloat16)
    key_valid = jnp.arange(TEXT, dtype=jnp.int32) < valid_length[0]

    def one_head(head_index):
        offset = (head_index * HD).astype(jnp.int32)
        query_part = lax.dynamic_slice_in_dim(query_normed, offset, HD, 1)
        key_part = lax.dynamic_slice_in_dim(key_normed, offset, HD, 1)
        value_part = lax.dynamic_slice_in_dim(value_proj, offset, HD, 1)
        scores = jnp.dot(query_part, key_part.T, preferred_element_type=jnp.float32) * HD ** (-0.5)
        scores = jnp.where(key_valid[None, :], scores, jnp.float32(-1e+30))
        shifted = jnp.exp(scores - lax.optimization_barrier(jnp.max(scores, axis=-1, keepdims=True)))
        weights = (shifted / lax.optimization_barrier(jnp.sum(shifted, axis=-1, keepdims=True))).astype(jnp.bfloat16)
        return jnp.dot(weights, value_part, preferred_element_type=jnp.float32).astype(jnp.bfloat16)
    per_head = lax.map(one_head, jnp.arange(HEADS, dtype=jnp.int32))
    attended = jnp.transpose(per_head, (1, 0, 2)).reshape(TOKENS, ATT)
    projected = jnp.dot(attended, out_weight, preferred_element_type=jnp.float32)
    residual_out = (video_rows.astype(jnp.float32) + projected).astype(jnp.bfloat16)
    half = FREQ // 2
    freqs = jnp.exp(-jnp.log(10000.0) * jnp.arange(half, dtype=jnp.float32) / half)
    angles = timestep[0].astype(jnp.float32) * freqs
    embedding = jnp.concatenate([jnp.cos(angles), jnp.sin(angles)])
    act = jax.nn.silu(embedding).astype(jnp.bfloat16)[None, :]
    shift = modulation[0] + jnp.dot(act, time_weight[0], preferred_element_type=jnp.float32)[0]
    scale = modulation[1] + jnp.dot(act, time_weight[1], preferred_element_type=jnp.float32)[0]
    resid = residual_out.astype(jnp.float32)
    mean2 = lax.optimization_barrier(jnp.mean(resid, axis=-1, keepdims=True))
    var2 = lax.optimization_barrier(jnp.mean(resid * resid, axis=-1, keepdims=True)) - mean2 * mean2
    modulated = ((resid - mean2) / jnp.sqrt(var2 + 1e-06) * (1.0 + scale) + shift).astype(jnp.bfloat16)
    return (residual_out, modulated)
```

```python
import functools

import jax
import jax.numpy as jnp
from jax import lax
from jax.experimental import pallas as pl
from jax.experimental.pallas import tpu as pltpu
from jax.sharding import Mesh
from jax.sharding import PartitionSpec as P

HD = 128
FREQ = 256
SEQ = ("x", "y")
DEV = pl.DeviceIdType.MESH
F32 = jnp.float32
BF16 = jnp.bfloat16


def remote(src, dst, send, recv, dev):
    return pltpu.make_async_remote_copy(
        src_ref=src, dst_ref=dst, send_sem=send, recv_sem=recv, device_id=dev, device_id_type=DEV
    )


class PlaneGather:
    def __init__(self, buf, send, recv, coords, a1, a2, r0, n):
        self.buf, self.send_sems, self.recv_sems = buf, send, recv
        self.a1, self.a2, self.p, self.q = a1, a2, coords[a1], coords[a2]
        self.whole, self.qa, self.qb = (r0, n), (r0, n // 2), (r0 + n // 2, n // 2)

    OFFS = (0, 3, 1, 2)

    def copy(self, idx, di, dq, rows, axis, step):
        i, j = lax.rem(self.p + di, 4), lax.rem(self.q + dq, 4)
        r = pl.ds(rows[0], rows[1])
        ref = self.buf.at[i, j, r] if self.a1 == "x" else self.buf.at[j, i, r]
        dev = {axis: lax.rem((self.p if axis == self.a1 else self.q) + step, 4)}
        return remote(ref, ref, self.send_sems.at[idx], self.recv_sems.at[idx], dev)

    def start(self):
        self.copy(0, 0, 0, self.whole, self.a1, 1).start()
        self.copy(1, 0, 0, self.whole, self.a1, 3).start()
        self.column(0)

    def column(self, i):
        self.copy(4 + 4 * i, self.OFFS[i], 0, self.whole, self.a2, 1).start()
        self.copy(5 + 4 * i, self.OFFS[i], 0, self.whole, self.a2, 3).start()

    def first(self):
        self.copy(0, 3, 0, self.whole, self.a1, 1).wait_recv()
        self.copy(2, 3, 0, self.qa, self.a1, 1).start()
        self.copy(1, 1, 0, self.whole, self.a1, 3).wait_recv()
        self.copy(3, 1, 0, self.qb, self.a1, 3).start()
        self.column(1)
        self.column(2)

    def pass_on(self, i):
        o = self.OFFS[i]
        self.copy(4 + 4 * i, o, 3, self.whole, self.a2, 1).wait_recv()
        self.copy(6 + 4 * i, o, 3, self.qa, self.a2, 1).start()
        self.copy(5 + 4 * i, o, 1, self.whole, self.a2, 3).wait_recv()
        self.copy(7 + 4 * i, o, 1, self.qb, self.a2, 3).start()

    def second(self):
        self.copy(2, 2, 0, self.qa, self.a1, 1).wait_recv()
        self.copy(3, 2, 0, self.qb, self.a1, 3).wait_recv()
        self.column(3)

    def finish(self):
        for i in range(4):
            o = self.OFFS[i]
            self.copy(6 + 4 * i, o, 2, self.qa, self.a2, 1).wait_recv()
            self.copy(7 + 4 * i, o, 2, self.qb, self.a2, 3).wait_recv()

    def wait_sends(self):
        self.copy(0, 0, 0, self.whole, self.a1, 1).wait_send()
        self.copy(1, 0, 0, self.whole, self.a1, 3).wait_send()
        self.copy(2, 3, 0, self.qa, self.a1, 1).wait_send()
        self.copy(3, 1, 0, self.qb, self.a1, 3).wait_send()
        for i in range(4):
            o = self.OFFS[i]
            self.copy(4 + 4 * i, o, 0, self.whole, self.a2, 1).wait_send()
            self.copy(5 + 4 * i, o, 0, self.whole, self.a2, 3).wait_send()
            self.copy(6 + 4 * i, o, 3, self.qa, self.a2, 1).wait_send()
            self.copy(7 + 4 * i, o, 1, self.qb, self.a2, 3).wait_send()


def diagonal(n):
    return lax.broadcasted_iota(jnp.int32, (n, n), 0) == lax.broadcasted_iota(jnp.int32, (n, n), 1)


def kernel(
    valid_ref, x_hbm, ctx_hbm, wq_hbm, wk_hbm, wv_hbm, wo_hbm, qg_ref, kg_ref,
    resid_ref, stat_ref,
    xv, nv, wq, wo, wo_own, ctxv, ctxs, ctxr, wkv, part, red, kv, vt, qt, att, acc, xt, gcol,
    ssk_own, ssk, ssq_own, ssq, st_own, st,
    load_sems, gq_s, gq_r, go_s, go_r, tp_s, tp_r, cx_s, cx_r, rd_s, rd_r, kv_s, kv_r,
    sk_s, sk_r, sq_s, sq_r, st_s, st_r, z_s, z_r, d_s, d_r,
):
    x, y, z, c = (lax.axis_index(a) for a in ("x", "y", "z", "c"))
    coords = {"x": x, "y": y}
    s, h = x * 4 + y, z * 2 + c
    tokens, width = xv.shape
    depth = width // 16
    heads = wq.shape[3]

    block = tokens // 8
    x_loads = [
        pltpu.make_async_copy(
            x_hbm.at[pl.ds(i * block, block)], xv.at[pl.ds(i * block, block)], load_sems.at[i]
        )
        for i in range(8)
    ]
    ctx_load = pltpu.make_async_copy(ctx_hbm, ctxv, load_sems.at[8])
    wq_load = pltpu.make_async_copy(wq_hbm, wq.at[x, y], load_sems.at[9])
    wk_load = pltpu.make_async_copy(
        wk_hbm, wkv.at[pl.ds(0, depth), pl.ds(0, heads)], load_sems.at[10]
    )
    wv_load = pltpu.make_async_copy(
        wv_hbm, wkv.at[pl.ds(0, depth), pl.ds(heads, heads)], load_sems.at[11]
    )
    wo_load = pltpu.make_async_copy(wo_hbm, wo_own, load_sems.at[12])
    ctx_load.start()
    wq_load.start()
    for load in x_loads:
        load.start()
    wk_load.start()
    wv_load.start()
    wo_load.start()

    barrier = pltpu.get_barrier_semaphore()

    def plane(k, sign=1):
        dx, dy = lax.div(k, 4), lax.rem(k, 4)
        if sign < 0:
            dx, dy = 4 - dx, 4 - dy
        return {"x": lax.rem(x + dx, 4), "y": lax.rem(y + dy, 4)}

    def line(k):
        return {"z": lax.rem(z + lax.div(k, 2), 8), "c": lax.rem(c + lax.rem(k, 2), 2)}

    partner = {"x": lax.div(h, 4), "y": lax.rem(h, 4), "z": lax.div(s, 2), "c": lax.rem(s, 2)}

    def each_peer(f):
        def step(k, carry):
            f(k)
            return carry

        lax.fori_loop(1, 16, step, 0)

    def greet(k):
        pl.semaphore_signal(barrier, inc=1, device_id=plane(k), device_id_type=DEV)
        pl.semaphore_signal(barrier, inc=1, device_id=line(k), device_id_type=DEV)

    each_peer(greet)

    @pl.when(s != h)
    def _():
        pl.semaphore_signal(barrier, inc=1, device_id=partner, device_id_type=DEV)

    def norm_rows(lo, hi):
        def step(i, carry):
            rows = pl.ds(pl.multiple_of(i * 16, 16), 16)
            v = xv[rows, :].astype(F32)
            mean = jnp.mean(v, axis=-1, keepdims=True)
            d = v - mean
            spread = jnp.mean(d * d, axis=-1, keepdims=True)
            nv[rows, :] = (d * (1.0 / jnp.sqrt(spread + 1e-06))).astype(BF16)
            return carry

        lax.fori_loop(lo // 16, hi // 16, step, 0)

    ctx_load.wait()
    for i in range(16):
        ctxs[i, :, 0:depth] = ctxv[:, i * depth : (i + 1) * depth]
        ctxs[i, :, depth:] = jnp.zeros((ctxs.shape[1], ctxs.shape[2] - depth), BF16)
    ctxr[0] = ctxs[s]
    wkv[depth:, :] = jnp.zeros((wkv.shape[0] - depth, wkv.shape[1]), BF16)
    wq_load.wait()
    x_loads[0].wait()
    x_loads[1].wait()
    norm_rows(0, 2 * block)

    @pl.when(s != h)
    def _():
        pl.semaphore_wait(barrier, 31)

    @pl.when(s == h)
    def _():
        pl.semaphore_wait(barrier, 30)

    def ctx_copy(k):
        dev = plane(k)
        return remote(
            ctxs.at[dev["x"] * 4 + dev["y"]], ctxr.at[k], cx_s.at[k], cx_r.at[k], dev
        )

    each_peer(lambda k: ctx_copy(k).start())

    half = wq.shape[2] // 2
    gq = [
        PlaneGather(wq, gq_s.at[0], gq_r.at[0], coords, "x", "y", 0, half),
        PlaneGather(wq, gq_s.at[1], gq_r.at[1], coords, "y", "x", half, half),
    ]
    for g in gq:
        g.start()

    x_loads[2].wait()
    norm_rows(2 * block, 3 * block)

    wk_load.wait()
    wv_load.wait()
    each_peer(lambda k: ctx_copy(k).wait_recv())
    rows = ctxr.shape[1]
    part[...] = jnp.dot(
        ctxr[...].reshape(16 * rows, ctxr.shape[2]), wkv[...], preferred_element_type=F32
    ).reshape(16, rows, 2 * heads)

    def red_copy(k):
        return remote(part.at[k], red.at[k], rd_s.at[k], rd_r.at[k], plane(k, -1))

    each_peer(lambda k: red_copy(k).start())
    for g in gq:
        g.first()

    for i in range(3, 8):
        x_loads[i].wait()
    norm_rows(3 * block, 6 * block)
    for g in gq:
        g.pass_on(0)
    norm_rows(6 * block, 8 * block)

    wo_load.wait()
    transpose = remote(wo_own, wo.at[partner["x"], partner["y"]], tp_s, tp_r, partner)
    stay = pltpu.make_async_copy(wo_own, wo.at[x, y], tp_r)

    @pl.when(s != h)
    def _():
        transpose.start()

    @pl.when(s == h)
    def _():
        stay.start()

    for g in gq:
        g.second()

    each_peer(lambda k: red_copy(k).wait_recv())
    total = part[0]
    for k in range(1, 16):
        total = total + red[k]
    key = total[:, :heads]
    eye = lax.broadcasted_iota(jnp.int32, (rows, 128), 0) == lax.broadcasted_iota(
        jnp.int32, (rows, 128), 1
    )
    key_sq = jnp.sum(key * key, axis=-1, keepdims=True)
    ssk_own[...] = jnp.sum(jnp.where(eye, key_sq, 0.0), axis=0, keepdims=True)

    def exchange(own, slots, send, recv):
        def copy(k):
            return remote(own, slots.at[k], send.at[k], recv.at[k], line(k))

        return copy

    sk_copy = exchange(ssk_own, ssk, sk_s, sk_r)
    each_peer(lambda k: sk_copy(k).start())
    for g in gq:
        g.pass_on(1)
        g.pass_on(2)
    kv[s, :, heads:] = total[:, heads:].astype(BF16)

    gcol[...] = jnp.broadcast_to(
        jnp.sum(jnp.where(diagonal(heads), qg_ref[...], 0.0), axis=1, keepdims=True), gcol.shape
    )
    xt[...] = xv[:, pl.ds(pl.multiple_of(z * (2 * depth), 128), 2 * depth)].T

    att_width = jnp.float32(16 * heads)
    each_peer(lambda k: sk_copy(k).wait_recv())
    sk_sum = ssk_own[...]
    for k in range(1, 16):
        sk_sum = sk_sum + ssk[k]
    key_rms = 1.0 / jnp.sqrt(sk_sum / att_width + 1e-06)
    key_scale = jnp.sum(jnp.where(eye, key_rms, 0.0), axis=-1, keepdims=True)
    kv[s, :, :heads] = (key * key_scale * kg_ref[...]).astype(BF16)

    def kv_copy(k):
        return remote(kv.at[s], kv.at[s], kv_s.at[k], kv_r.at[k], plane(k))

    def kv_wait(k):
        dev = plane(k, -1)
        src = dev["x"] * 4 + dev["y"]
        return remote(kv.at[src], kv.at[src], kv_s.at[k], kv_r.at[k], dev)

    each_peer(lambda k: kv_copy(k).start())
    for g in gq:
        g.pass_on(3)
    for g in gq:
        g.finish()

    for i in range(4):
        piece = jnp.dot(
            nv[:, i * 4 * depth : (i + 1) * 4 * depth],
            wq[i].reshape(4 * depth, heads),
            preferred_element_type=F32,
        )
        if i == 0:
            acc_q = piece
        else:
            acc_q = acc_q + piece
    qt[...] = acc_q.T
    ssq_own[...] = jnp.sum(qt[...] * qt[...], axis=0, keepdims=True)
    sq_copy = exchange(ssq_own, ssq, sq_s, sq_r)
    each_peer(lambda k: sq_copy(k).start())

    @pl.when(s != h)
    def _():
        transpose.wait_recv()
        transpose.wait_send()

    @pl.when(s == h)
    def _():
        stay.wait()

    go = [
        PlaneGather(wo, go_s.at[0], go_r.at[0], coords, "x", "y", 0, half),
        PlaneGather(wo, go_s.at[1], go_r.at[1], coords, "y", "x", half, half),
    ]
    for g in go:
        g.start()

    each_peer(lambda k: kv_wait(k).wait_recv())
    text = 16 * rows
    vt[...] = kv[:, :, heads:].reshape(text, heads).T

    each_peer(lambda k: sq_copy(k).wait_recv())
    sq_sum = ssq_own[...]
    for k in range(1, 16):
        sq_sum = sq_sum + ssq[k]
    query_rms = 1.0 / jnp.sqrt(sq_sum / att_width + 1e-06)

    valid = valid_ref[0]
    cols = 256

    def z_copy(flow, d, j, own):
        step = 1 if flow == 0 else 7
        back = (8 - d) if flow == 0 else d
        if own:
            back = (8 - d + 1) if flow == 0 else d - 1
        src = lax.rem(z + back, 8)
        ref = att.at[src, c, j]
        return remote(
            ref, ref, z_s.at[flow, d, j], z_r.at[flow, d, j], {"z": lax.rem(z + step, 8)}
        )

    def d_copy(flow, d, j, own):
        back = (8 - d) if flow == 0 else d
        src = lax.rem(z + back, 8)
        ref = att.at[src, c if own else 1 - c, j]
        return remote(ref, ref, d_s.at[flow, d, j], d_r.at[flow, d, j], {"c": 1 - c})

    for j in range(heads // HD):
        for t in range(tokens // cols):
            tok = slice(t * cols, (t + 1) * cols)
            hd = slice(j * HD, (j + 1) * HD)
            query = (
                qt[hd, tok] * query_rms[:, tok] * jnp.broadcast_to(gcol[hd, 0:1], (HD, cols))
            ).astype(BF16)
            keys = kv[:, :, hd].reshape(text, HD)
            scores = jnp.dot(keys, query, preferred_element_type=F32) * HD ** (-0.5)
            ok = lax.broadcasted_iota(jnp.int32, (text, cols), 0) < valid
            scores = jnp.where(ok, scores, -1e30)
            shifted = jnp.exp(scores - jnp.max(scores, axis=0, keepdims=True))
            weights = (shifted * (1.0 / jnp.sum(shifted, axis=0, keepdims=True))).astype(BF16)
            att[z, c, j, :, tok] = jnp.dot(
                vt[hd, :], weights, preferred_element_type=F32
            ).astype(BF16)
        z_copy(0, 1, j, True).start()
        z_copy(1, 1, j, True).start()
        d_copy(0, 0, j, True).start()
        if j == 0:
            for g in go:
                g.first()

    for g in go:
        g.pass_on(0)
    for g in go:
        g.second()
    for g in go:
        g.pass_on(1)
        g.pass_on(2)

    def project(zz, cc, first=False):
        src = zz * 2 + cc
        w = wo[lax.div(src, 4), lax.rem(src, 4)]
        term = jnp.dot(w, att[zz, cc].reshape(heads, tokens), preferred_element_type=F32)
        acc[...] = term if first else acc[...] + term

    def forward(d):
        for j in range(2):
            for flow in range(2):
                z_copy(flow, d, j, False).wait_recv()
                if d < 3 or j == flow:
                    z_copy(flow, d + 1, j, True).start()
                d_copy(flow, d, j, True).start()

    def add_in(d):
        for flow in range(2):
            zz = lax.rem(z + ((8 - d) if flow == 0 else d), 8)
            for j in range(2):
                d_copy(flow, d, j, False).wait_recv()
            project(zz, c)
            project(zz, 1 - c)

    forward(1)
    for g in go:
        g.pass_on(3)
    for g in go:
        g.finish()
    for j in range(2):
        d_copy(0, 0, j, False).wait_recv()
    project(z, c, True)
    project(z, 1 - c)
    forward(2)
    add_in(1)
    forward(3)
    add_in(2)
    add_in(3)
    far = lax.rem(z + 4, 8)
    for j in range(2):
        z_copy(j, 4, j, False).wait_recv()
        d_copy(j, 4, j, True).start()
    for j in range(2):
        d_copy(j, 4, j, False).wait_recv()
    project(far, c)
    project(far, 1 - c)

    resid = (xt[pl.ds(pl.multiple_of(c * depth, 16), depth), :].astype(F32) + acc[...]).astype(BF16)
    resid_ref[...] = resid
    wide = resid.astype(F32)
    st_own[0:1, :] = jnp.sum(wide, axis=0, keepdims=True)
    st_own[1:2, :] = jnp.sum(wide * wide, axis=0, keepdims=True)
    st_copy = exchange(st_own, st, st_s, st_r)
    each_peer(lambda k: st_copy(k).start())

    def drain(k):
        ctx_copy(k).wait_send()
        red_copy(k).wait_send()
        sk_copy(k).wait_send()
        kv_copy(k).wait_send()
        sq_copy(k).wait_send()

    each_peer(drain)
    for g in gq + go:
        g.wait_sends()
    for flow in range(2):
        for d in range(1, 5):
            for j in range(2):
                if d < 4 or j == flow:
                    z_copy(flow, d, j, True).wait_send()
                    d_copy(flow, d, j, True).wait_send()
    for j in range(2):
        d_copy(0, 0, j, True).wait_send()

    each_peer(lambda k: st_copy(k).wait_recv())
    stats = st_own[...]
    for k in range(1, 16):
        stats = stats + st[k]
    mean2 = stats[0:1, :] / width
    var2 = stats[1:2, :] / width - mean2 * mean2
    stat_ref[0:1, :] = mean2
    stat_ref[1:2, :] = 1.0 / jnp.sqrt(var2 + 1e-06)
    each_peer(lambda k: st_copy(k).wait_send())


def fused(valid_length, video, context, wq, wk, wv, wo_t, query_gain, key_gain):
    tokens, width = video.shape
    depth, heads = wq.shape
    rows = context.shape[0]
    pad = -(-depth // 128) * 128
    dma = pltpu.SemaphoreType.DMA
    any_spec = pl.BlockSpec(memory_space=pl.ANY)
    vmem = pl.BlockSpec(memory_space=pltpu.VMEM)
    return pl.pallas_call(
        kernel,
        out_shape=(
            jax.ShapeDtypeStruct((depth, tokens), BF16),
            jax.ShapeDtypeStruct((2, tokens), F32),
        ),
        in_specs=[pl.BlockSpec(memory_space=pltpu.SMEM)] + [any_spec] * 6 + [vmem] * 2,
        out_specs=(vmem, vmem),
        scratch_shapes=[
            pltpu.VMEM((tokens, width), BF16),
            pltpu.VMEM((tokens, width), BF16),
            pltpu.VMEM((4, 4, depth, heads), BF16),
            pltpu.VMEM((4, 4, depth, heads), BF16),
            pltpu.VMEM((depth, heads), BF16),
            pltpu.VMEM((rows, width), BF16),
            pltpu.VMEM((16, rows, pad), BF16),
            pltpu.VMEM((16, rows, pad), BF16),
            pltpu.VMEM((pad, 2 * heads), BF16),
            pltpu.VMEM((16, rows, 2 * heads), F32),
            pltpu.VMEM((16, rows, 2 * heads), F32),
            pltpu.VMEM((16, rows, 2 * heads), BF16),
            pltpu.VMEM((heads, 16 * rows), BF16),
            pltpu.VMEM((heads, tokens), F32),
            pltpu.VMEM((8, 2, heads // HD, HD, tokens), BF16),
            pltpu.VMEM((depth, tokens), F32),
            pltpu.VMEM((2 * depth, tokens), BF16),
            pltpu.VMEM((heads, 128), F32),
            pltpu.VMEM((1, 128), F32),
            pltpu.VMEM((16, 1, 128), F32),
            pltpu.VMEM((1, tokens), F32),
            pltpu.VMEM((16, 1, tokens), F32),
            pltpu.VMEM((2, tokens), F32),
            pltpu.VMEM((16, 2, tokens), F32),
            dma((13,)),
            dma((2, 20)), dma((2, 20)), dma((2, 20)), dma((2, 20)),
            dma, dma,
            dma((16,)), dma((16,)), dma((16,)), dma((16,)), dma((16,)), dma((16,)),
            dma((16,)), dma((16,)), dma((16,)), dma((16,)), dma((16,)), dma((16,)),
            dma((2, 5, 2)), dma((2, 5, 2)), dma((2, 5, 2)), dma((2, 5, 2)),
        ],
        compiler_params=pltpu.CompilerParams(
            collective_id=0, has_side_effects=True, vmem_limit_bytes=60 * 1024 * 1024
        ),
        name="cross",
    )(valid_length, video, context, wq, wk, wv, wo_t, query_gain[None, :], key_gain[None, :])


def on_device(
    video_rows,
    context,
    valid_length,
    timestep,
    query_weight,
    key_weight,
    value_weight,
    out_weight,
    query_gain,
    key_gain,
    time_weight,
    modulation,
):
    resid_t, stats = fused(
        valid_length, video_rows, context, query_weight, key_weight, value_weight, out_weight.T,
        query_gain, key_gain,
    )
    half = FREQ // 2
    freqs = jnp.exp(-jnp.log(10000.0) * jnp.arange(half, dtype=F32) / half)
    angles = timestep[0].astype(F32) * freqs
    embedding = jnp.concatenate([jnp.cos(angles), jnp.sin(angles)])
    act = jax.nn.silu(embedding).astype(BF16)[None, :]
    shift = modulation[0] + jnp.dot(act, time_weight[0], preferred_element_type=F32)[0]
    scale = modulation[1] + jnp.dot(act, time_weight[1], preferred_element_type=F32)[0]
    resid = resid_t.astype(F32)
    modulated = (
        (resid - stats[0:1]) * stats[1:2] * (1.0 + scale)[:, None] + shift[:, None]
    ).astype(BF16)
    return resid_t.T, modulated.T


def solution(mesh):
    split = Mesh(mesh.devices.reshape(4, 4, 8, 2), ("x", "y", "z", "c"))
    line = ("z", "c")
    return jax.shard_map(
        on_device,
        mesh=split,
        in_specs=(
            P(SEQ, None),
            P(SEQ, None),
            P(),
            P(),
            P(SEQ, line),
            P(SEQ, line),
            P(SEQ, line),
            P(line, SEQ),
            P(line),
            P(line),
            P(None, None, line),
            P(None, line),
        ),
        out_specs=(P(SEQ, line), P(SEQ, line)),
        check_vma=False,
    )
```
